128 devices in a mesh: batch: 1, col: 16 (over z, y), row: 8 (over x, core).
Axes of the slice: x: 4, y: 4, z: 4, core: 2. Of those that a mesh axis runs over, the one named last changes fastest.
Arguments:
- tri_mat: float32 [8192, 8192], P(('batch', 'row'), 'col')
Outputs:
- output: float32 [8192, 8192], P(('batch', 'row'), 'col')
All inputs are finite; a program needn't handle non-finite values.
Results may differ from the reference program's by a relative error of at most 0.001.
Values sent between devices are 32-bit elements.
A program may use at most 1 GiB of HBM per device.

```python
import jax
import jax.numpy as jnp
from jax import lax

N = 8192
LEAF_MAX = 512


def setup_inputs(seed: int = 0, part: int = 0) -> dict:
    base_key = jax.random.fold_in(jax.random.key(seed), part)
    key_diag, key_low = jax.random.split(base_key)
    diag_vals = jax.random.uniform(key_diag, (N,), jnp.float32, 2.0, 4.0)
    low_vals = jax.random.normal(key_low, (N, N), jnp.float32) * (1.5 * N ** -0.5)
    tri_mat = jnp.tril(low_vals, -1) + jnp.diag(diag_vals)
    return {"tri_mat": tri_mat}


def mat_prod(left_mat, right_mat):
    return jnp.dot(left_mat, right_mat, precision=lax.Precision.HIGHEST, preferred_element_type=jnp.float32)


def tri_inverse(tri_block):
    mat_size = tri_block.shape[0]
    if mat_size <= LEAF_MAX:
        eye_mat = jnp.eye(mat_size, dtype=jnp.float32)
        return lax.linalg.triangular_solve(tri_block, eye_mat, left_side=True, lower=True)
    half_size = mat_size // 2
    inv_top = tri_inverse(tri_block[:half_size, :half_size])
    inv_bot = tri_inverse(tri_block[half_size:, half_size:])
    cross_prod = mat_prod(tri_block[half_size:, :half_size], inv_top)
    lower_left = -mat_prod(inv_bot, cross_prod)
    top_rows = jnp.concatenate([inv_top, jnp.zeros((half_size, half_size), jnp.float32)], axis=1)
    bot_rows = jnp.concatenate([lower_left, inv_bot], axis=1)
    return jnp.concatenate([top_rows, bot_rows], axis=0)


def reference(tri_mat):
    return tri_inverse(tri_mat)
```

```python
import jax
import jax.numpy as jnp
from jax import lax
from jax.experimental import pallas as pl
from jax.experimental.pallas import tpu as pltpu
from jax.sharding import Mesh, PartitionSpec as P

F32 = jnp.float32
AXES = ("z", "y", "x", "core")
NZ, NY, NX, NK = 4, 4, 4, 2
COORDS = [(z, y, x, k) for z in range(NZ) for y in range(NY) for x in range(NX) for k in range(NK)]
INDEX = {c: i for i, c in enumerate(COORDS)}
LEAF, BASE, SUB = 512, 128, 128


def dot(left, right):
    return jnp.dot(left, right, precision=lax.Precision.HIGHEST, preferred_element_type=F32)


def dot_blocks(left, right):
    return lax.dot_general(left, right, (((0, 2), (0, 1)), ((), ())), precision=lax.Precision.HIGHEST, preferred_element_type=F32)


def leaf_kernel(m_ref, o_ref):
    rows = lax.broadcasted_iota(jnp.int32, (BASE, BASE), 0)
    cols = lax.broadcasted_iota(jnp.int32, (BASE, BASE), 1)
    eye = (rows == cols).astype(F32)
    o_ref[...] = jnp.zeros_like(o_ref)
    powers, sums, recips = [], [], []
    for b in range(LEAF // BASE):
        s = slice(b * BASE, (b + 1) * BASE)
        blk = m_ref[s, s]
        diag = jnp.where(rows == cols, blk, 0.0)
        recip_col = 1.0 / jnp.sum(diag, axis=1, keepdims=True)
        recips.append(1.0 / jnp.sum(diag, axis=0, keepdims=True))
        strict = jnp.where(rows > cols, blk, 0.0) * recip_col
        sums.append(eye - strict)
        powers.append(dot(strict, strict))
    steps = BASE.bit_length() - 2
    for i in range(steps):
        sums = [p + dot(p, q) for p, q in zip(sums, powers)]
        if i < steps - 1:
            powers = [dot(q, q) for q in powers]
    for b in range(LEAF // BASE):
        s = slice(b * BASE, (b + 1) * BASE)
        o_ref[s, s] = sums[b] * recips[b]
    size = BASE
    while size < LEAF:
        prods = []
        for lo in range(0, LEAF, 2 * size):
            a, c = slice(lo, lo + size), slice(lo + size, lo + 2 * size)
            prods.append((a, c, dot(m_ref[c, a], o_ref[a, a])))
        for a, c, t in prods:
            o_ref[c, a] = -dot(o_ref[c, c], t)
        size *= 2


def leaf_inverse(half):
    return pl.pallas_call(
        leaf_kernel,
        out_shape=jax.ShapeDtypeStruct((LEAF, LEAF), F32),
        in_specs=[pl.BlockSpec(memory_space=pltpu.VMEM)],
        out_specs=pl.BlockSpec(memory_space=pltpu.VMEM),
        cost_estimate=pl.CostEstimate(flops=20_000_000, bytes_accessed=2_000_000, transcendentals=0),
    )(half)


def route(tile, rule):
    pairs = []
    for c in COORDS:
        dest = rule(*c)
        if dest is not None:
            pairs.append((INDEX[c], INDEX[dest]))
    return lax.ppermute(tile, AXES, pairs)


def invert(t):
    z, y, x, k = (lax.axis_index(a) for a in AXES)
    on_diag = z == x
    leaf0 = on_diag & (y == 2 * k)
    leaf1 = on_diag & (y == 2 * k + 1)
    x_odd = x % 2 == 1

    c3 = jnp.zeros((LEAF, SUB), F32)
    for h in range(2):
        for q in range(4):
            piece = t[h * LEAF:(h + 1) * LEAF, q * SUB:(q + 1) * SUB]
            c3 = c3 + route(piece, lambda zz, yy, xx, kk, h=h, q=q: (q, yy, xx - h, kk) if xx % 2 == 1 and zz == xx - 1 else None)
    g3 = lax.all_gather(c3, ("z", "y"), axis=0)
    c4 = jnp.zeros((LEAF, 2 * SUB), F32)
    for h in range(2):
        for p in range(2):
            piece = t[h * LEAF:(h + 1) * LEAF, p * 2 * SUB:(p + 1) * 2 * SUB]
            c4 = c4 + route(piece, lambda zz, yy, xx, kk, h=h, p=p: (3 - zz if p else zz, yy, 3 - xx if h else xx, kk) if xx >= 2 and zz < 2 else None)
    g4 = lax.all_gather(c4, ("z", "y"), axis=0)

    rows = lax.broadcasted_iota(jnp.int32, (LEAF, LEAF), 0)
    cols = lax.broadcasted_iota(jnp.int32, (LEAF, LEAF), 1)
    eye = (rows == cols).astype(F32)
    half = jnp.where(leaf0, t[:LEAF], jnp.where(leaf1, t[LEAF:], eye))
    inv = leaf_inverse(half)

    inv_next = route(inv, lambda zz, yy, xx, kk: (zz, yy - 1, xx, kk) if zz == xx and yy == 2 * kk + 1 else None)
    x10 = -dot(inv_next, dot(t[LEAF:], inv))
    zero = jnp.zeros((LEAF, LEAF), F32)
    ecol = jnp.concatenate([jnp.where(leaf0, inv, zero), jnp.where(leaf0, x10, jnp.where(leaf1, inv, zero))], axis=0)

    c_other = route(t, lambda zz, yy, xx, kk: (zz, 1 - yy, xx, kk) if zz == xx and yy < 2 and kk == 1 else None)
    first, second = jnp.where(y == 0, t, c_other), jnp.where(y == 0, c_other, t)
    acol = route(ecol, lambda zz, yy, xx, kk: (zz, yy, xx, 1) if zz == xx and yy < 2 and kk == 0 else None)
    t2 = dot(first, acol[:LEAF]) + dot(second, acol[LEAF:])
    near = route(inv, lambda zz, yy, xx, kk: (zz, {2: 1, 3: 0}[yy], xx, kk) if zz == xx and yy >= 2 and kk == 1 else None)
    far = route(inv, lambda zz, yy, xx, kk: (zz, {2: 0, 3: 1}[yy], xx, kk) if zz == xx and yy >= 2 and kk == 1 else None)
    inv2 = jnp.where(y == 0, far, near)
    inv3 = jnp.where(y == 0, near, far)
    x32 = route(x10, lambda zz, yy, xx, kk: (zz, 1, xx, kk) if zz == xx and yy == 2 and kk == 1 else None) \
        + route(x10, lambda zz, yy, xx, kk: (zz, 0, xx, kk) if zz == xx and yy == 2 and kk == 1 else None)
    top = dot(inv2, t2[:LEAF])
    bot = dot(x32, t2[:LEAF]) + dot(inv3, t2[LEAF:])
    low = jnp.concatenate([-top, -bot], axis=0)
    dg = jnp.where(on_diag & (k == 1) & (y < 2), low, ecol)

    dq = jnp.zeros((2 * LEAF, SUB), F32)
    for q in range(4):
        dq = dq + route(dg[:, q * SUB:(q + 1) * SUB], lambda zz, yy, xx, kk, q=q: (q, yy, xx, kk) if zz == xx else None)

    def by_zy(mat):
        return mat.reshape(4, 4, SUB, mat.shape[1]).transpose(1, 0, 2, 3).reshape(16, SUB, mat.shape[1])

    lower = dq[LEAF:]
    d3 = jnp.where(x_odd, dq[:LEAF], route(lower, lambda zz, yy, xx, kk: (zz, yy, xx - 1, kk) if xx % 2 == 1 else None))
    gd3 = lax.all_gather(d3, ("z", "y"), axis=0)
    d_flip = route(dq, lambda zz, yy, xx, kk: (zz, yy, xx, 1 - kk) if xx % 2 == 0 else None)
    d_hop = route(dq, lambda zz, yy, xx, kk: (zz, yy, xx + 1, kk) if xx % 2 == 0 else None)
    d_both = route(dq, lambda zz, yy, xx, kk: (zz, yy, xx + 1, 1 - kk) if xx % 2 == 0 else None)
    own = jnp.where(x_odd, d_hop, dq)
    other = jnp.where(x_odd, d_both, d_flip)
    ds = jnp.concatenate([jnp.where(k == 0, own, other), jnp.where(k == 0, other, own)], axis=0)
    t3 = dot_blocks(g3, by_zy(ds))
    t3_k = route(t3, lambda zz, yy, xx, kk: (zz, yy, xx, 1 - kk))
    t3_x = route(t3, lambda zz, yy, xx, kk: (zz, yy, xx ^ 1, kk))
    t3_xk = route(t3, lambda zz, yy, xx, kk: (zz, yy, xx ^ 1, 1 - kk))

    def part(odd, core):
        same_x = x_odd if odd else jnp.logical_not(x_odd)
        same_k = k == core
        return jnp.where(same_x, jnp.where(same_k, t3, t3_k), jnp.where(same_k, t3_x, t3_xk))

    t3_full = jnp.concatenate([part(True, 0), part(False, 0), part(True, 1), part(False, 1)], axis=0)
    x3 = -dot_blocks(gd3, by_zy(t3_full))

    team_d = lax.all_gather(dq, ("x", "core"), axis=0)
    team_x = lax.all_gather(x3, ("x", "core"), axis=0)
    d0 = team_d[0:2].reshape(2048, SUB)
    d1 = team_d[2:4].reshape(2048, SUB)
    x10s = jnp.concatenate([team_x[2], team_x[0], team_x[3], team_x[1]], axis=0)
    a_top = jnp.concatenate([d0, jnp.zeros_like(d0)], axis=1)
    a_bot = jnp.concatenate([x10s, d1], axis=1)
    a_mat = jnp.concatenate([a_top, a_bot], axis=0).reshape(2, 4, 2, 2 * SUB, 2 * SUB)
    a_blocks = jnp.stack([a_mat[0, :, 0], a_mat[1, :, 0], a_mat[1, :, 1], a_mat[0, :, 1]]).reshape(16, 2 * SUB, 2 * SUB)
    t4 = dot_blocks(g4, a_blocks)
    inner = (x == 1) | (x == 2)
    dt = jnp.where(x >= 2, dq[:LEAF], route(lower, lambda zz, yy, xx, kk: (zz, yy, 3 - xx, kk) if xx >= 2 else None))
    xt = jnp.where(x == 3, x3, route(x3, lambda zz, yy, xx, kk: (zz, yy, 0, kk) if xx == 2 else None))
    g_second = lax.all_gather(jnp.where(inner, 0.0, dt), ("z", "y"), axis=0)
    g_first = lax.all_gather(jnp.where(inner, dt, xt), ("z", "y"), axis=0)
    team_t = lax.all_gather(t4, ("x", "core"), axis=0)
    t_first = jnp.concatenate([team_t[4], team_t[2], team_t[5], team_t[3]], axis=0)
    t_second = jnp.concatenate([team_t[6], team_t[0], team_t[7], team_t[1]], axis=0)
    x4 = -(dot_blocks(g_first, by_zy(t_first)) + dot_blocks(g_second, by_zy(t_second)))

    out = dg
    pieces = []
    for h in range(2):
        row = []
        for q in range(4):
            got = route(x3, lambda zz, yy, xx, kk, h=h, q=q: (xx | 1) - 1 >= 0 and (((xx | 1) - 1), yy, xx | 1, kk) if zz == q and (xx % 2 == 1) == (h == 0) else None)
            for j in range(2):
                got = got + route(x4[:, j * SUB:(j + 1) * SUB], lambda zz, yy, xx, kk, h=h, q=q, j=j: (j, yy, xx if h == 0 else 3 - xx, kk) if zz == q and (xx >= 2) == (h == 0) else None)
            row.append(got)
        pieces.append(jnp.concatenate(row, axis=1))
    return out + jnp.concatenate(pieces, axis=0)


def solution(mesh):
    grid = Mesh(mesh.devices.reshape(NZ, NY, NX, NK), AXES)
    spec = P(("x", "core"), ("z", "y"))
    return jax.shard_map(invert, mesh=grid, in_specs=(spec,), out_specs=spec, check_vma=False)
```

```python
import functools

import jax
import jax.numpy as jnp
from jax import lax
from jax.experimental import pallas as pl
from jax.experimental.pallas import tpu as pltpu
from jax.sharding import Mesh, PartitionSpec as P

F32 = jnp.float32
AXES = ("z", "y", "x", "core")
RING = 4
SUB = 128
LEAF = 4 * SUB
MESH = pl.DeviceIdType.MESH
VMEM = pl.BlockSpec(memory_space=pltpu.VMEM)


def dot(left, right):
    return jnp.dot(left, right, precision=lax.Precision.HIGHEST, preferred_element_type=F32)


def dot_blocks(left, right):
    return lax.dot_general(left, right, (((0, 2), (0, 1)), ((), ())), precision=lax.Precision.HIGHEST, preferred_element_type=F32)


def here():
    return tuple(lax.axis_index(a) for a in AXES)


def turn(i, d):
    return lax.rem(i + d + RING, RING)


def enter(peers):
    barrier = pltpu.get_barrier_semaphore()
    for peer in peers:
        pl.semaphore_signal(barrier, inc=1, device_id=peer, device_id_type=MESH)
    pl.semaphore_wait(barrier, len(peers))


def call(kernel, shapes, scratch, ident, *args):
    return pl.pallas_call(
        kernel,
        out_shape=[jax.ShapeDtypeStruct(s, F32) for s in shapes],
        in_specs=[VMEM] * len(args),
        out_specs=[VMEM] * len(shapes),
        scratch_shapes=scratch,
        compiler_params=pltpu.CompilerParams(collective_id=ident, has_side_effects=True),
        name=kernel.__name__,
    )(*args)


def sems(n):
    return [pltpu.SemaphoreType.DMA((n,)), pltpu.SemaphoreType.DMA((n,))]


class Link:
    def __init__(self, send, recv, base=0):
        self.send, self.recv, self.base = send, recv, base

    def copy(self, i, src, dst, dev, recv=None):
        j = i if recv is None else recv
        return pltpu.make_async_remote_copy(
            src_ref=src, dst_ref=dst, send_sem=self.send.at[self.base + i], recv_sem=self.recv.at[self.base + j], device_id=dev, device_id_type=MESH
        )


def matmul(out, left, right, sign=1.0, add=None, rows=2 * SUB):
    def step(i, _):
        tile = pl.ds(pl.multiple_of(i * rows, rows), rows)
        prod = dot(left[tile, :], right[...])
        prod = prod if sign > 0 else -prod
        out[tile, :] = prod if add is None else add[tile, :] + prod
        return 0

    lax.fori_loop(0, left.shape[0] // rows, step, 0)


def invert_leaf(m_ref, o_ref):
    rows = lax.broadcasted_iota(jnp.int32, (SUB, SUB), 0)
    cols = lax.broadcasted_iota(jnp.int32, (SUB, SUB), 1)
    eye = (rows == cols).astype(F32)
    o_ref[...] = jnp.zeros(o_ref.shape, F32)
    powers, sums, recips = [], [], []
    for b in range(LEAF // SUB):
        s = slice(b * SUB, (b + 1) * SUB)
        blk = m_ref[s, s]
        diag = jnp.where(rows == cols, blk, 0.0)
        recip_col = 1.0 / jnp.sum(diag, axis=1, keepdims=True)
        recips.append(1.0 / jnp.sum(diag, axis=0, keepdims=True))
        strict = jnp.where(rows > cols, blk, 0.0) * recip_col
        sums.append(eye - strict)
        powers.append(dot(strict, strict))
    steps = SUB.bit_length() - 2
    for i in range(steps):
        sums = [p + dot(p, q) for p, q in zip(sums, powers)]
        if i < steps - 1:
            powers = [dot(q, q) for q in powers]
    for b in range(LEAF // SUB):
        s = slice(b * SUB, (b + 1) * SUB)
        o_ref[s, s] = sums[b] * recips[b]
    size = SUB
    while size < LEAF:
        prods = []
        for lo in range(0, LEAF, 2 * size):
            a, c = slice(lo, lo + size), slice(lo + size, lo + 2 * size)
            prods.append((a, c, dot(m_ref[c, a], o_ref[a, a])))
        for a, c, t in prods:
            o_ref[c, a] = -dot(o_ref[c, c], t)
        size *= 2


def leaves(t_ref, inv, nb, near, l_next, c_next, c3, c4, m_ref, send, recv, local):
    z, y, x, k = here()
    link = Link(send, recv)
    on = z == x
    mine = on & (y // 2 == k)
    pair_y = y + 1 - 2 * lax.rem(y, 2)
    peers = [{"z": turn(z, d), "x": px} for px in (x, 3 - x) for d in range(RING) if not (d == 0 and px is x)]
    peers += [{"y": turn(y, d)} for d in range(1, RING)]
    enter(peers)
    low = slice(LEAF, 2 * LEAF)
    c_src, l_src = on & (k == 1) & (y == 1), on & (k == 1) & (y == 2)
    c_copy = link.copy(0, t_ref, c_next, {"y": turn(y, -1)})
    l_copy = link.copy(1, t_ref.at[low, :], l_next, {"y": turn(y, 1)})
    pl.when(c_src)(lambda: c_copy.start())
    pl.when(l_src)(lambda: l_copy.start())

    src3 = (lax.rem(x, 2) == 1) & (z == x - 1)
    copies3 = []
    for h in range(2):
        for d in range(RING):
            q = turn(z, d)
            piece = t_ref.at[h * LEAF:(h + 1) * LEAF, pl.ds(pl.multiple_of(q * SUB, SUB), SUB)]
            if h == 0 and d == 0:
                own3 = pltpu.make_async_copy(piece, c3, local.at[0])
            else:
                copies3.append(link.copy(4 + len(copies3), piece, c3, {"z": q, "x": 3 - x if h else x}, recv=4))

    @pl.when(src3)
    def _():
        for c in copies3:
            c.start()
        own3.start()

    src4 = (x >= 2) & (z < 2)
    copies4 = []
    for h in range(2):
        for p in range(2):
            piece = t_ref.at[h * LEAF:(h + 1) * LEAF, 2 * SUB * p:2 * SUB * (p + 1)]
            if h == 0 and p == 0:
                own4 = pltpu.make_async_copy(piece, c4, local.at[1])
            else:
                copies4.append(link.copy(11 + len(copies4), piece, c4, {"z": 3 - z if p else z, "x": 3 - x if h else x}, recv=5))

    @pl.when(src4)
    def _():
        for c in copies4:
            c.start()
        own4.start()

    inv_pair = link.copy(2, inv, nb, {"y": pair_y})
    inv_near = link.copy(3, inv, near, {"y": 3 - y})
    near_src, near_dst = on & (k == 1) & (y >= 2), on & (k == 1) & (y < 2)

    @pl.when(mine)
    def _():
        half = pl.ds(pl.multiple_of(lax.rem(y, 2) * LEAF, LEAF), LEAF)
        m_ref[...] = t_ref[half, :]
        invert_leaf(m_ref, inv)
        inv_pair.start()
        pl.when(near_src)(lambda: inv_near.start())
        inv_pair.wait()
        pl.when(near_src)(lambda: inv_near.wait_send())

    pl.when(near_dst)(lambda: inv_near.wait_recv())
    pl.when(c_src)(lambda: c_copy.wait_send())
    pl.when(l_src)(lambda: l_copy.wait_send())
    pl.when(on & (k == 1) & (y == 0))(lambda: c_copy.wait_recv())
    pl.when(on & (k == 1) & (y == 3))(lambda: l_copy.wait_recv())

    @pl.when(src3)
    def _():
        for c in copies3:
            c.wait_send()
        own3.wait()

    @pl.when(src4)
    def _():
        for c in copies4:
            c.wait_send()
        own4.wait()

    pl.when(jnp.logical_not(src3))(lambda: copies3[0].wait_recv())
    pl.when(jnp.logical_not(src4))(lambda: link.copy(11, t_ref.at[:LEAF, :2 * SUB], c4, {"z": z}, recv=5).wait_recv())


def diagonal(t_ref, inv, nb, near, l_next, c_next, dg, x10, a_buf, far, x32, tmp, prod, send, recv):
    z, y, x, k = here()
    link = Link(send, recv)
    enter([{"y": turn(y, d)} for d in range(1, RING)] + [{"core": 1 - k}])
    low, up = slice(LEAF, 2 * LEAF), slice(0, LEAF)

    @pl.when(z == x)
    def _():
        dg[...] = jnp.zeros(dg.shape, F32)
        fwd = link.copy(0, nb, far, {"y": 3 - y})
        a_first = link.copy(1, inv, a_buf.at[0], {"core": 1 - k})
        a_second = link.copy(2, x10, a_buf.at[1], {"core": 1 - k})
        x_far = link.copy(3, x10, x32, {"y": 3 - y})
        b_side, a_side, work = (k == 1) & (y >= 2), (k == 0) & (y < 2), (k == 1) & (y < 2)
        pl.when(b_side)(lambda: fwd.start())
        pl.when(a_side)(lambda: a_first.start())

        @pl.when(y == 2 * k)
        def _():
            matmul(tmp, t_ref.at[low, :], inv)
            matmul(x10, nb, tmp, -1.0)
            pl.when(k == 0)(lambda: a_second.start())
            pl.when(k == 1)(lambda: x_far.start())
            dg[up, :] = inv[...]
            dg[low, :] = x10[...]

        @pl.when((k == 1) & (y == 3))
        def _():
            matmul(tmp, l_next, nb)
            matmul(x10, inv, tmp, -1.0)
            x_far.start()

        @pl.when(y == 2 * k + 1)
        def _():
            dg[low, :] = inv[...]

        @pl.when(work)
        def _():
            a_first.wait_recv()
            matmul(prod, t_ref, a_buf.at[0])

            @pl.when(y == 0)
            def _():
                a_second.wait_recv()
                matmul(prod, c_next, a_buf.at[1], add=prod)
                matmul(dg.at[low, :], near, prod.at[low, :], -1.0)
                fwd.wait_recv()
                matmul(dg.at[up, :], far, prod.at[up, :], -1.0)

            @pl.when(y == 1)
            def _():
                matmul(dg.at[up, :], near, prod.at[up, :], -1.0)
                fwd.wait_recv()
                matmul(dg.at[low, :], far, prod.at[low, :], -1.0)

            x_far.wait_recv()
            matmul(dg.at[low, :], x32, prod.at[up, :], -1.0, add=dg.at[low, :])

        @pl.when(b_side)
        def _():
            fwd.wait_send()
            x_far.wait_send()

        pl.when(a_side)(lambda: a_first.wait_send())
        pl.when((k == 0) & (y == 0))(lambda: a_second.wait_send())


def run(*stages):
    stages = list(stages)
    while stages:
        for s in list(stages):
            try:
                next(s)
            except StopIteration:
                stages.remove(s)


def ring_stages(link, axis, pos, block, spare):
    left, right = {axis: turn(pos, -1)}, {axis: turn(pos, 1)}
    own = block(pos)
    to_right, to_left = link.copy(0, own, own, right), link.copy(1, own, own, left)
    to_right.start()
    to_left.start()
    yield
    from_left, from_right = block(turn(pos, -1)), block(turn(pos, 1))
    link.copy(0, from_left, from_left, right).wait_recv()
    half0 = spare(turn(pos, -1), 0)
    on_right = link.copy(2, half0, half0, right)
    on_right.start()
    link.copy(1, from_right, from_right, left).wait_recv()
    half1 = spare(turn(pos, 1), 1)
    on_left = link.copy(3, half1, half1, left)
    on_left.start()
    yield
    far0, far1 = spare(turn(pos, 2), 0), spare(turn(pos, 2), 1)
    link.copy(2, far0, far0, right).wait_recv()
    link.copy(3, far1, far1, left).wait_recv()
    for c in (to_right, to_left, on_right, on_left):
        c.wait_send()


def plane_gather(ref, z, y, send, recv, base):
    n = ref.shape[2]
    spans = [pl.ds(c * (n // 2), n // 2) for c in range(2)]

    def quarter(c, half):
        return pl.ds(c * (n // 2) + half * (n // 4), n // 4)

    first = [
        ring_stages(Link(send, recv, base), "y", y, lambda i: ref.at[z, i, spans[0], :], lambda i, h: ref.at[z, i, quarter(0, h), :]),
        ring_stages(Link(send, recv, base + 4), "z", z, lambda i: ref.at[i, y, spans[1], :], lambda i, h: ref.at[i, y, quarter(1, h), :]),
    ]
    for _ in range(2):
        for s in first:
            next(s)
        yield
    for s in first:
        next(s, None)
    second = [
        ring_stages(Link(send, recv, base + 8), "z", z, lambda i: ref.at[i, :, spans[0], :], lambda i, h: ref.at[i, :, quarter(0, h), :]),
        ring_stages(Link(send, recv, base + 12), "y", y, lambda i: ref.at[:, i, spans[1], :], lambda i, h: ref.at[:, i, quarter(1, h), :]),
    ]
    for _ in range(2):
        for s in second:
            next(s)
        yield
    for s in second:
        next(s, None)


def team_gather(ref, x, k, send, recv, base):
    link = Link(send, recv, base)
    n = ref.shape[1]
    halves = [pl.ds(h * (n // 2), n // 2) for h in range(2)]
    left, right, flip = {"x": turn(x, -1)}, {"x": turn(x, 1)}, {"core": 1 - k}

    def blk(d, core):
        return ref.at[2 * turn(x, d) + core]

    def part(d, core, h):
        return ref.at[2 * turn(x, d) + core, halves[h], :]

    def same(i, view, dev):
        return link.copy(i, view, view, dev)

    sent = [same(0, blk(0, k), right), same(1, blk(0, k), left), same(2, blk(0, k), flip)]
    for c in sent:
        c.start()
    yield
    same(0, blk(-1, k), right).wait_recv()
    more = [same(3, part(-1, k, 0), right), same(4, blk(-1, k), flip)]
    for c in more:
        c.start()
    sent += more
    same(1, blk(1, k), left).wait_recv()
    more = [same(5, part(1, k, 1), left), same(6, blk(1, k), flip)]
    for c in more:
        c.start()
    sent += more
    yield
    same(3, part(2, k, 0), right).wait_recv()
    more = [same(7, part(2, k, 0), flip)]
    same(5, part(2, k, 1), left).wait_recv()
    more.append(same(8, part(2, k, 1), flip))
    for c in more:
        c.start()
    sent += more
    yield
    same(2, blk(0, 1 - k), flip).wait_recv()
    same(4, blk(-1, 1 - k), flip).wait_recv()
    same(6, blk(1, 1 - k), flip).wait_recv()
    same(7, part(2, 1 - k, 0), flip).wait_recv()
    same(8, part(2, 1 - k, 1), flip).wait_recv()
    for c in sent:
        c.wait_send()


def ring_peers(*axes):
    return [{a: turn(lax.axis_index(a), d)} for a in axes for d in (1, -1)]


def spread(dg, team, hop, rows, send, recv, local):
    z, y, x, k = here()
    link = Link(send, recv)
    enter([{"z": turn(z, d)} for d in range(1, RING)] + ring_peers("y", "x") + [{"core": 1 - k}])
    slot = 2 * x + k

    def column(q):
        return dg.at[:, pl.ds(pl.multiple_of(q * SUB, SUB), SUB)]

    out = [link.copy(d, column(turn(z, d)), team.at[slot], {"z": turn(z, d)}, recv=0) for d in range(1, RING)]
    own = pltpu.make_async_copy(column(z), team.at[slot], local.at[0])

    @pl.when(z == x)
    def _():
        for c in (out[0], out[2], out[1]):
            c.start()
        own.start()
        own.wait()

    pl.when(z != x)(lambda: out[0].wait_recv())
    cross = link.copy(4, team.at[slot, LEAF:, :], hop, {"x": 3 - x})
    cross.start()
    gather = team_gather(team, x, k, send, recv, 5)
    next(gather)
    take = pltpu.make_async_copy(team.at[slot, :LEAF, :], rows.at[z, y], local.at[1])
    odd = lax.rem(x, 2) == 1

    @pl.when(odd)
    def _():
        take.start()
        take.wait()

    cross.wait_recv()
    take_hop = pltpu.make_async_copy(hop, rows.at[z, y], local.at[1])

    @pl.when(jnp.logical_not(odd))
    def _():
        take_hop.start()
        take_hop.wait()

    run(plane_gather(rows, z, y, send, recv, 14), gather)
    cross.wait_send()

    @pl.when(z == x)
    def _():
        for c in out:
            c.wait_send()


def swap(t_ref, full, send, recv, local):
    z, y, x, k = here()
    link = Link(send, recv)
    enter([{"x": 3 - x}, {"core": 1 - k}])
    even = 1 - lax.rem(x, 2)
    mine, theirs = 2 * k + even, 2 * k + 1 - even
    cross = link.copy(0, t_ref, full.at[mine], {"x": 3 - x})
    flip = link.copy(1, t_ref, full.at[mine], {"core": 1 - k})
    own = pltpu.make_async_copy(t_ref, full.at[mine], local.at[0])
    for c in (cross, flip, own):
        c.start()
    cross.wait_recv()
    on = link.copy(2, full.at[theirs], full.at[theirs], {"core": 1 - k})
    on.start()
    own.wait()
    flip.wait_recv()
    on.wait_recv()
    for c in (cross, flip, on):
        c.wait_send()


def team_only(tile, team, send, recv, local):
    z, y, x, k = here()
    enter(ring_peers("x") + [{"core": 1 - k}])
    own = pltpu.make_async_copy(tile, team.at[2 * x + k], local.at[0])
    own.start()
    own.wait()
    run(team_gather(team, x, k, send, recv, 0))


def team_and_plane(tile, block, team, plane, send, recv, local):
    z, y, x, k = here()
    enter(ring_peers("z", "y", "x") + [{"core": 1 - k}])
    own = pltpu.make_async_copy(tile, team.at[2 * x + k], local.at[0])
    own_block = pltpu.make_async_copy(block, plane.at[z, y], local.at[1])
    own.start()
    own_block.start()
    own.wait()
    own_block.wait()
    run(plane_gather(plane, z, y, send, recv, 9), team_gather(team, x, k, send, recv, 0))


def place(dg, x3, x4, out, send, recv, local):
    z, y, x, k = here()
    link = Link(send, recv)
    peers = [{"z": turn(z, d), "x": px} for px in (x, 3 - x) for d in range(RING) if not (d == 0 and px is x)]
    enter(peers)

    def spot(h, q):
        return out.at[pl.ds(pl.multiple_of(h * LEAF, LEAF), LEAF), pl.ds(pl.multiple_of(q * SUB, SUB), SUB)]

    odd = lax.rem(x, 2) == 1
    h3 = jnp.where(odd, 0, 1)
    i3 = jnp.where(odd, x, 3 - x)
    h4 = jnp.where(x >= 2, 0, 1)
    i4 = jnp.where(x >= 2, x, 3 - x)
    jobs = [(x3, h3, i3, i3 - 1)] + [(x4.at[:, j * SUB:(j + 1) * SUB], h4, i4, j) for j in range(2)]
    for n, (src, h, i, zz) in enumerate(jobs):
        stay = (i == x) & (zz == z)
        go = pltpu.make_async_remote_copy(
            src_ref=src, dst_ref=spot(h, z), send_sem=send.at[n], recv_sem=recv.at[h * RING + z], device_id={"z": zz, "x": i}, device_id_type=MESH
        )
        keep = pltpu.make_async_copy(src, spot(h, z), local.at[0])
        pl.when(jnp.logical_not(stay))(lambda go=go: go.start())
        pl.when(stay)(lambda keep=keep: keep.start())

    keep_d = pltpu.make_async_copy(dg, out, local.at[1])

    @pl.when(z == x)
    def _():
        keep_d.start()
        keep_d.wait()

    @pl.when(z > x)
    def _():
        out[...] = jnp.zeros(out.shape, F32)

    target = (odd & (z == x - 1)) | ((x >= 2) & (z < 2))

    @pl.when(target)
    def _():
        for h in range(2):
            for d in range(RING):
                q = turn(z, d)
                if h == 0 and d == 0:
                    pltpu.make_async_copy(x3, spot(0, z), local.at[0]).wait()
                else:
                    pltpu.make_async_remote_copy(
                        src_ref=x3, dst_ref=spot(h, q), send_sem=send.at[0], recv_sem=recv.at[h * RING + q], device_id={"z": z}, device_id_type=MESH
                    ).wait_recv()

    for n, (src, h, i, zz) in enumerate(jobs):
        stay = (i == x) & (zz == z)
        go = pltpu.make_async_remote_copy(
            src_ref=src, dst_ref=spot(h, z), send_sem=send.at[n], recv_sem=recv.at[h * RING + z], device_id={"z": zz, "x": i}, device_id_type=MESH
        )
        pl.when(jnp.logical_not(stay))(lambda go=go: go.wait_send())


def by_zy(mat):
    n = mat.shape[1]
    return mat.reshape(RING, RING, SUB, n).transpose(1, 0, 2, 3).reshape(RING * RING, SUB, n)


def invert(t):
    x, k = lax.axis_index("x"), lax.axis_index("core")
    inner = (x == 1) | (x == 2)
    dma2 = pltpu.SemaphoreType.DMA((2,))
    leaf, tile = (LEAF, LEAF), (2 * LEAF, LEAF)
    inv, nb, near, l_next, c_next, c3, c4 = call(
        leaves, [leaf, leaf, leaf, leaf, tile, (LEAF, SUB), (LEAF, 2 * SUB)], [pltpu.VMEM(leaf, F32)] + sems(14) + [dma2], 0, t
    )
    g3 = lax.all_gather(c3, ("z", "y"), axis=0)
    g4 = lax.all_gather(c4, ("z", "y"), axis=0)
    scratch = [pltpu.VMEM(leaf, F32), pltpu.VMEM((2,) + leaf, F32), pltpu.VMEM(leaf, F32), pltpu.VMEM(leaf, F32), pltpu.VMEM(leaf, F32), pltpu.VMEM(tile, F32)]
    (dg,) = call(diagonal, [tile], scratch + sems(4), 1, t, inv, nb, near, l_next, c_next)
    team_d, hop, rows3 = call(spread, [(8, 2 * LEAF, SUB), (LEAF, SUB), (RING, RING, LEAF, SUB)], sems(30) + [dma2], 2, dg)
    rows3 = rows3.reshape(16, LEAF, SUB)

    ds = lax.dynamic_slice_in_dim(team_d, jnp.where(inner, 0, 4), 2, axis=0).reshape(4 * LEAF, SUB)
    t3 = dot_blocks(g3, by_zy(ds))
    (t3_full,) = call(swap, [(4, LEAF, SUB)], sems(3) + [dma2], 3, t3)
    x3 = -dot_blocks(rows3, by_zy(t3_full.reshape(4 * LEAF, SUB)))

    (team_x,) = call(team_only, [(8, LEAF, SUB)], sems(9) + [dma2], 4, x3)
    d0 = team_d[0:2].reshape(4 * LEAF, SUB)
    d1 = team_d[2:4].reshape(4 * LEAF, SUB)
    x10s = jnp.concatenate([team_x[2], team_x[4], team_x[3], team_x[5]], axis=0)
    a_top = jnp.concatenate([d0, jnp.zeros_like(d0)], axis=1)
    a_bot = jnp.concatenate([x10s, d1], axis=1)
    a_mat = jnp.concatenate([a_top, a_bot], axis=0).reshape(2, RING, 2, 2 * SUB, 2 * SUB)
    a_blocks = jnp.stack([a_mat[0, :, 0], a_mat[1, :, 0], a_mat[1, :, 1], a_mat[0, :, 1]]).reshape(16, 2 * SUB, 2 * SUB)
    t4 = dot_blocks(g4, a_blocks)
    d2_rows = jnp.where(x == 2, lax.dynamic_index_in_dim(team_d, 4 + k, axis=0, keepdims=False)[:LEAF], hop)
    first_rows = jnp.where(inner, d2_rows, x3)
    team_t, rows4 = call(team_and_plane, [(8, LEAF, 2 * SUB), (RING, RING, LEAF, SUB)], sems(25) + [dma2], 5, t4, first_rows)
    rows4 = rows4.reshape(16, LEAF, SUB)
    t_first = jnp.concatenate([team_t[4], team_t[2], team_t[5], team_t[3]], axis=0)
    t_second = jnp.where(inner, 0.0, jnp.concatenate([team_t[6], team_t[0], team_t[7], team_t[1]], axis=0))
    x4 = -(dot_blocks(rows4, by_zy(t_first)) + dot_blocks(rows3, by_zy(t_second)))
    (out,) = call(place, [tile], [pltpu.SemaphoreType.DMA((3,)), pltpu.SemaphoreType.DMA((8,)), dma2], 6, dg, x3, x4)
    return out


def solution(mesh):
    grid = Mesh(mesh.devices.reshape(RING, RING, RING, 2), AXES)
    spec = P(("x", "core"), ("z", "y"))
    return jax.shard_map(invert, mesh=grid, in_specs=(spec,), out_specs=spec, check_vma=False)
```

```python
import functools

import jax
import jax.numpy as jnp
from jax import lax
from jax.experimental import pallas as pl
from jax.experimental.pallas import tpu as pltpu
from jax.sharding import Mesh, PartitionSpec as P

F32 = jnp.float32
AXES = ("z", "y", "x", "core")
RING = 4
SUB = 128
LEAF = 4 * SUB
MESH = pl.DeviceIdType.MESH
VMEM = pl.BlockSpec(memory_space=pltpu.VMEM)


def dot(left, right):
    return jnp.dot(left, right, precision=lax.Precision.HIGHEST, preferred_element_type=F32)


def dot_blocks(left, right):
    return lax.dot_general(left, right, (((0, 2), (0, 1)), ((), ())), precision=lax.Precision.HIGHEST, preferred_element_type=F32)


def here():
    return tuple(lax.axis_index(a) for a in AXES)


def turn(i, d):
    return lax.rem(i + d + RING, RING)


def enter(peers):
    barrier = pltpu.get_barrier_semaphore()
    for peer in peers:
        pl.semaphore_signal(barrier, inc=1, device_id=peer, device_id_type=MESH)
    pl.semaphore_wait(barrier, len(peers))


def call(kernel, shapes, scratch, ident, *args):
    return pl.pallas_call(
        kernel,
        out_shape=[jax.ShapeDtypeStruct(s, F32) for s in shapes],
        in_specs=[VMEM] * len(args),
        out_specs=[VMEM] * len(shapes),
        scratch_shapes=scratch,
        compiler_params=pltpu.CompilerParams(collective_id=ident, has_side_effects=True),
        name=kernel.__name__,
    )(*args)


def sems(n):
    return [pltpu.SemaphoreType.DMA((n,)), pltpu.SemaphoreType.DMA((n,))]


class Link:
    def __init__(self, send, recv, base=0):
        self.send, self.recv, self.base = send, recv, base

    def copy(self, i, src, dst, dev, recv=None):
        j = i if recv is None else recv
        return pltpu.make_async_remote_copy(
            src_ref=src, dst_ref=dst, send_sem=self.send.at[self.base + i], recv_sem=self.recv.at[self.base + j], device_id=dev, device_id_type=MESH
        )


def matmul(out, left, right, sign=1.0, add=None, rows=2 * SUB):
    def step(i, _):
        tile = pl.ds(pl.multiple_of(i * rows, rows), rows)
        prod = dot(left[tile, :], right[...])
        prod = prod if sign > 0 else -prod
        out[tile, :] = prod if add is None else add[tile, :] + prod
        return 0

    lax.fori_loop(0, left.shape[0] // rows, step, 0)


def invert_leaf(m_ref, o_ref):
    rows = lax.broadcasted_iota(jnp.int32, (SUB, SUB), 0)
    cols = lax.broadcasted_iota(jnp.int32, (SUB, SUB), 1)
    eye = (rows == cols).astype(F32)
    o_ref[...] = jnp.zeros(o_ref.shape, F32)
    powers, sums, recips = [], [], []
    for b in range(LEAF // SUB):
        s = slice(b * SUB, (b + 1) * SUB)
        blk = m_ref[s, s]
        diag = jnp.where(rows == cols, blk, 0.0)
        recip_col = 1.0 / jnp.sum(diag, axis=1, keepdims=True)
        recips.append(1.0 / jnp.sum(diag, axis=0, keepdims=True))
        strict = jnp.where(rows > cols, blk, 0.0) * recip_col
        sums.append(eye - strict)
        powers.append(dot(strict, strict))
    steps = SUB.bit_length() - 2
    for i in range(steps):
        sums = [p + dot(p, q) for p, q in zip(sums, powers)]
        if i < steps - 1:
            powers = [dot(q, q) for q in powers]
    for b in range(LEAF // SUB):
        s = slice(b * SUB, (b + 1) * SUB)
        o_ref[s, s] = sums[b] * recips[b]
    size = SUB
    while size < LEAF:
        prods = []
        for lo in range(0, LEAF, 2 * size):
            a, c = slice(lo, lo + size), slice(lo + size, lo + 2 * size)
            prods.append((a, c, dot(m_ref[c, a], o_ref[a, a])))
        for a, c, t in prods:
            o_ref[c, a] = -dot(o_ref[c, c], t)
        size *= 2


def strips(link, i, src, dst, dev):
    spans = [(slice(b * SUB, (b + 1) * SUB), slice(0, (b + 1) * SUB)) for b in range(LEAF // SUB)]
    return [link.copy(i + b, src.at[r, c], dst.at[r, c], dev) for b, (r, c) in enumerate(spans)]


def start(copies):
    for c in copies:
        c.start()


def sent(copies):
    for c in copies:
        c.wait_send()


def arrived(copies):
    for c in copies:
        c.wait_recv()


def diagonal(t_ref, dg, dq, c3, c4, m_ref, inv, nb, bi, ai, l_up, l_side, ax, tt, x32, x10, tmp, prod, send, recv, local):
    z, y, x, k = here()
    link = Link(send, recv)
    on = z == x
    low, up = slice(LEAF, 2 * LEAF), slice(0, LEAF)
    mine = on & (y // 2 == k)
    first = y < 2
    role_a, role_b, tail = on & (k == 0) & first, on & (k == 1) & first, on & (k == 1) & jnp.logical_not(first)
    y0, y1, y2, y3 = y == 0, y == 1, y == 2, y == 3

    for buf in (nb, bi, ai, dg):
        buf[...] = jnp.zeros(buf.shape, F32)
    peers = [{"z": turn(z, d), "x": px} for px in (x, 3 - x) for d in range(RING) if not (d == 0 and px is x)]
    peers += [{"y": turn(y, d), "core": c} for d in range(1, RING) for c in (0, 1)] + [{"core": 1 - k}]
    enter(peers)

    l21 = [link.copy(0, t_ref.at[up, :], l_side, {"y": 0, "core": 0})]
    l_d2d = [link.copy(1, t_ref.at[up, :], l_up, {"core": 1 - k})]
    l31 = [link.copy(2, t_ref.at[low, :], l_side, {"y": 0, "core": 1})]
    l32 = [link.copy(3, t_ref.at[low, :], l_side, {"y": 3, "core": 1})]

    @pl.when(role_b & y1)
    def _():
        start(l21)
        start(l31)

    pl.when(role_b)(lambda: start(l_d2d))
    pl.when(tail & y2)(lambda: start(l32))

    src3 = (lax.rem(x, 2) == 1) & (z == x - 1)
    copies3 = []
    for h in range(2):
        for d in range(RING):
            q = turn(z, d)
            piece = t_ref.at[h * LEAF:(h + 1) * LEAF, pl.ds(pl.multiple_of(q * SUB, SUB), SUB)]
            if h == 0 and d == 0:
                own3 = pltpu.make_async_copy(piece, c3, local.at[0])
            else:
                copies3.append(link.copy(30 + len(copies3), piece, c3, {"z": q, "x": 3 - x if h else x}, recv=30))

    @pl.when(src3)
    def _():
        start(copies3)
        own3.start()

    src4 = (x >= 2) & (z < 2)
    copies4 = []
    for h in range(2):
        for p in range(2):
            piece = t_ref.at[h * LEAF:(h + 1) * LEAF, 2 * SUB * p:2 * SUB * (p + 1)]
            if h == 0 and p == 0:
                own4 = pltpu.make_async_copy(piece, c4, local.at[1])
            else:
                copies4.append(link.copy(37 + len(copies4), piece, c4, {"z": 3 - z if p else z, "x": 3 - x if h else x}, recv=37))

    @pl.when(src4)
    def _():
        start(copies4)
        own4.start()

    def column(rows, q):
        return dg.at[rows, pl.ds(pl.multiple_of(q * SUB, SUB), SUB)]

    def scatter(rows, i):
        return [link.copy(i + d - 1, column(rows, turn(z, d)), dq.at[rows, :], {"z": turn(z, d)}, recv=i) for d in (1, 3, 2)]

    go_up, go_low = scatter(up, 24), scatter(low, 27)
    keep_up = pltpu.make_async_copy(column(up, z), dq.at[up, :], local.at[2])
    keep_low = pltpu.make_async_copy(column(low, z), dq.at[low, :], local.at[3])

    def emit_up():
        start(go_up)
        keep_up.start()

    def emit_low():
        start(go_low)
        keep_low.start()

    pair = strips(link, 4, inv, nb, {"y": y + 1 - 2 * lax.rem(y, 2)})
    near = strips(link, 8, inv, bi, {"y": 3 - y, "core": lax.rem(y, 2)})
    forward = strips(link, 12, nb, bi, {"y": 3 - y, "core": 1 - lax.rem(y, 2)})
    a_inv = strips(link, 16, inv, ai, {"core": 1 - k})
    a_x = [link.copy(20, x10, ax, {"core": 1 - k})]
    t_top = [link.copy(21, prod, tt, {"core": 1 - k})]
    x_far = [link.copy(22, x10, x32, {"y": 3 - y})]
    res_up = [link.copy(23, tmp, dg.at[up, :], {"core": 1 - k})]

    @pl.when(mine)
    def _():
        half = pl.ds(pl.multiple_of(lax.rem(y, 2) * LEAF, LEAF), LEAF)
        m_ref[...] = t_ref[half, :]
        invert_leaf(m_ref, inv)
        start(pair)
        dg[half, :] = inv[...]

        @pl.when(k == 1)
        def _():
            start(near)

        @pl.when(k == 0)
        def _():
            start(a_inv)

    @pl.when(on & (k == 0) & jnp.logical_not(first))
    def _():
        emit_up()
        emit_low()

    @pl.when(role_a)
    def _():
        emit_up()
        pl.when(y1)(emit_low)
        arrived(l_d2d)
        matmul(prod, l_up, inv)

        @pl.when(y0)
        def _():
            matmul(tmp, t_ref.at[low, :], inv)
            arrived(pair)
            matmul(x10, nb, tmp, -1.0)
            start(a_x)
            dg[low, :] = x10[...]
            emit_low()
            arrived(l21)
            matmul(prod, l_side, x10, add=prod)

        start(t_top)
        pl.when(y0)(lambda: arrived(forward))
        pl.when(y1)(lambda: arrived(near))
        matmul(tmp, bi, prod, -1.0)
        start(res_up)
        pl.when(y1)(lambda: arrived(pair))

    @pl.when(tail)
    def _():
        emit_up()

        @pl.when(y2)
        def _():
            matmul(tmp, t_ref.at[low, :], inv)
            arrived(pair)
            start(forward)
            matmul(x10, nb, tmp, -1.0)
            start(x_far)
            dg[low, :] = x10[...]
            emit_low()

        @pl.when(y3)
        def _():
            emit_low()
            arrived(pair)
            start(forward)
            arrived(l32)
            matmul(tmp, l_side, nb)
            matmul(x10, inv, tmp, -1.0)
            start(x_far)

    @pl.when(role_b)
    def _():
        arrived(a_inv)
        matmul(prod, t_ref.at[low, :], ai)

        @pl.when(y0)
        def _():
            arrived(a_x)
            arrived(l31)
            matmul(prod, l_side, ax, add=prod)
            arrived(near)

        pl.when(y1)(lambda: arrived(forward))
        matmul(dg.at[low, :], bi, prod, -1.0)
        arrived(res_up)
        emit_up()
        arrived(t_top)
        arrived(x_far)
        matmul(dg.at[low, :], x32, tt, -1.0, add=dg.at[low, :])
        emit_low()

    pl.when(mine)(lambda: sent(pair))

    @pl.when(role_a)
    def _():
        sent(a_inv + t_top + res_up)
        pl.when(y0)(lambda: sent(a_x))

    @pl.when(role_b)
    def _():
        sent(l_d2d)
        pl.when(y1)(lambda: sent(l21 + l31))

    @pl.when(tail)
    def _():
        sent(near + forward + x_far)
        pl.when(y2)(lambda: sent(l32))

    @pl.when(on)
    def _():
        sent(go_up + go_low)
        keep_up.wait()
        keep_low.wait()

    @pl.when(jnp.logical_not(on))
    def _():
        go_up[0].wait_recv()
        go_low[0].wait_recv()

    @pl.when(src3)
    def _():
        sent(copies3)
        own3.wait()

    @pl.when(src4)
    def _():
        sent(copies4)
        own4.wait()

    pl.when(jnp.logical_not(src3))(lambda: copies3[0].wait_recv())
    pl.when(jnp.logical_not(src4))(lambda: copies4[0].wait_recv())


def run(*stages):
    stages = list(stages)
    while stages:
        for s in list(stages):
            try:
                next(s)
            except StopIteration:
                stages.remove(s)


def ring_stages(link, axis, pos, block, spare):
    left, right = {axis: turn(pos, -1)}, {axis: turn(pos, 1)}
    own = block(pos)
    to_right, to_left = link.copy(0, own, own, right), link.copy(1, own, own, left)
    to_right.start()
    to_left.start()
    yield
    from_left, from_right = block(turn(pos, -1)), block(turn(pos, 1))
    link.copy(0, from_left, from_left, right).wait_recv()
    half0 = spare(turn(pos, -1), 0)
    on_right = link.copy(2, half0, half0, right)
    on_right.start()
    link.copy(1, from_right, from_right, left).wait_recv()
    half1 = spare(turn(pos, 1), 1)
    on_left = link.copy(3, half1, half1, left)
    on_left.start()
    yield
    far0, far1 = spare(turn(pos, 2), 0), spare(turn(pos, 2), 1)
    link.copy(2, far0, far0, right).wait_recv()
    link.copy(3, far1, far1, left).wait_recv()
    for c in (to_right, to_left, on_right, on_left):
        c.wait_send()


def plane_gather(ref, z, y, send, recv, base):
    n = ref.shape[2]
    spans = [pl.ds(c * (n // 2), n // 2) for c in range(2)]

    def quarter(c, half):
        return pl.ds(c * (n // 2) + half * (n // 4), n // 4)

    first = [
        ring_stages(Link(send, recv, base), "y", y, lambda i: ref.at[z, i, spans[0], :], lambda i, h: ref.at[z, i, quarter(0, h), :]),
        ring_stages(Link(send, recv, base + 4), "z", z, lambda i: ref.at[i, y, spans[1], :], lambda i, h: ref.at[i, y, quarter(1, h), :]),
    ]
    for _ in range(2):
        for s in first:
            next(s)
        yield
    for s in first:
        next(s, None)
    second = [
        ring_stages(Link(send, recv, base + 8), "z", z, lambda i: ref.at[i, :, spans[0], :], lambda i, h: ref.at[i, :, quarter(0, h), :]),
        ring_stages(Link(send, recv, base + 12), "y", y, lambda i: ref.at[:, i, spans[1], :], lambda i, h: ref.at[:, i, quarter(1, h), :]),
    ]
    for _ in range(2):
        for s in second:
            next(s)
        yield
    for s in second:
        next(s, None)


def team_gather(ref, x, k, send, recv, base):
    link = Link(send, recv, base)
    n = ref.shape[1]
    halves = [pl.ds(h * (n // 2), n // 2) for h in range(2)]
    left, right, flip = {"x": turn(x, -1)}, {"x": turn(x, 1)}, {"core": 1 - k}

    def blk(d, core):
        return ref.at[2 * turn(x, d) + core]

    def part(d, core, h):
        return ref.at[2 * turn(x, d) + core, halves[h], :]

    def same(i, view, dev):
        return link.copy(i, view, view, dev)

    sent = [same(0, blk(0, k), right), same(1, blk(0, k), left), same(2, blk(0, k), flip)]
    for c in sent:
        c.start()
    yield
    same(0, blk(-1, k), right).wait_recv()
    more = [same(3, part(-1, k, 0), right), same(4, blk(-1, k), flip)]
    for c in more:
        c.start()
    sent += more
    same(1, blk(1, k), left).wait_recv()
    more = [same(5, part(1, k, 1), left), same(6, blk(1, k), flip)]
    for c in more:
        c.start()
    sent += more
    yield
    same(3, part(2, k, 0), right).wait_recv()
    more = [same(7, part(2, k, 0), flip)]
    same(5, part(2, k, 1), left).wait_recv()
    more.append(same(8, part(2, k, 1), flip))
    for c in more:
        c.start()
    sent += more
    yield
    same(2, blk(0, 1 - k), flip).wait_recv()
    same(4, blk(-1, 1 - k), flip).wait_recv()
    same(6, blk(1, 1 - k), flip).wait_recv()
    same(7, part(2, 1 - k, 0), flip).wait_recv()
    same(8, part(2, 1 - k, 1), flip).wait_recv()
    for c in sent:
        c.wait_send()


def ring_peers(*axes):
    return [{a: turn(lax.axis_index(a), d)} for a in axes for d in (1, -1)]


def spread(dq, c3, team, hop, rows, g3, send, recv, local):
    z, y, x, k = here()
    link = Link(send, recv)
    enter(ring_peers("z", "y", "x") + [{"core": 1 - k}])
    slot = 2 * x + k
    cross = link.copy(0, dq.at[LEAF:, :], hop, {"x": 3 - x})
    cross.start()
    own = pltpu.make_async_copy(dq, team.at[slot], local.at[0])
    own3 = pltpu.make_async_copy(c3, g3.at[z, y], local.at[1])
    own.start()
    own3.start()
    own3.wait()
    panel = plane_gather(g3, z, y, send, recv, 26)
    next(panel)
    own.wait()
    gather = team_gather(team, x, k, send, recv, 1)
    next(gather)
    odd = lax.rem(x, 2) == 1
    take = pltpu.make_async_copy(dq.at[:LEAF, :], rows.at[z, y], local.at[2])
    take_hop = pltpu.make_async_copy(hop, rows.at[z, y], local.at[2])
    cross.wait_recv()
    pl.when(odd)(lambda: take.start())
    pl.when(jnp.logical_not(odd))(lambda: take_hop.start())
    take.wait()
    run(plane_gather(rows, z, y, send, recv, 10), panel, gather)
    cross.wait_send()


def swap(t_ref, full, send, recv, local):
    z, y, x, k = here()
    link = Link(send, recv)
    enter([{"x": 3 - x}, {"core": 1 - k}])
    even = 1 - lax.rem(x, 2)
    mine, theirs = 2 * k + even, 2 * k + 1 - even
    cross = link.copy(0, t_ref, full.at[mine], {"x": 3 - x})
    flip = link.copy(1, t_ref, full.at[mine], {"core": 1 - k})
    own = pltpu.make_async_copy(t_ref, full.at[mine], local.at[0])
    for c in (cross, flip, own):
        c.start()
    cross.wait_recv()
    on = link.copy(2, full.at[theirs], full.at[theirs], {"core": 1 - k})
    on.start()
    own.wait()
    flip.wait_recv()
    on.wait_recv()
    for c in (cross, flip, on):
        c.wait_send()


def team_only(tile, team, send, recv, local):
    z, y, x, k = here()
    enter(ring_peers("x") + [{"core": 1 - k}])
    own = pltpu.make_async_copy(tile, team.at[2 * x + k], local.at[0])
    own.start()
    own.wait()
    run(team_gather(team, x, k, send, recv, 0))


def team_and_plane(tile, block, team, plane, send, recv, local):
    z, y, x, k = here()
    enter(ring_peers("z", "y", "x") + [{"core": 1 - k}])
    own = pltpu.make_async_copy(tile, team.at[2 * x + k], local.at[0])
    own_block = pltpu.make_async_copy(block, plane.at[z, y], local.at[1])
    own.start()
    own_block.start()
    own.wait()
    own_block.wait()
    run(plane_gather(plane, z, y, send, recv, 9), team_gather(team, x, k, send, recv, 0))


def place(dg, x3, x4, out, send, recv, local):
    z, y, x, k = here()
    link = Link(send, recv)
    peers = [{"z": turn(z, d), "x": px} for px in (x, 3 - x) for d in range(RING) if not (d == 0 and px is x)]
    enter(peers)

    def spot(h, q):
        return out.at[pl.ds(pl.multiple_of(h * LEAF, LEAF), LEAF), pl.ds(pl.multiple_of(q * SUB, SUB), SUB)]

    odd = lax.rem(x, 2) == 1
    h3 = jnp.where(odd, 0, 1)
    i3 = jnp.where(odd, x, 3 - x)
    h4 = jnp.where(x >= 2, 0, 1)
    i4 = jnp.where(x >= 2, x, 3 - x)
    jobs = [(x3, h3, i3, i3 - 1)] + [(x4.at[:, j * SUB:(j + 1) * SUB], h4, i4, j) for j in range(2)]
    for n, (src, h, i, zz) in enumerate(jobs):
        stay = (i == x) & (zz == z)
        go = pltpu.make_async_remote_copy(
            src_ref=src, dst_ref=spot(h, z), send_sem=send.at[n], recv_sem=recv.at[h * RING + z], device_id={"z": zz, "x": i}, device_id_type=MESH
        )
        keep = pltpu.make_async_copy(src, spot(h, z), local.at[0])
        pl.when(jnp.logical_not(stay))(lambda go=go: go.start())
        pl.when(stay)(lambda keep=keep: keep.start())

    keep_d = pltpu.make_async_copy(dg, out, local.at[1])

    @pl.when(z == x)
    def _():
        keep_d.start()
        keep_d.wait()

    @pl.when(z > x)
    def _():
        out[...] = jnp.zeros(out.shape, F32)

    target = (odd & (z == x - 1)) | ((x >= 2) & (z < 2))

    @pl.when(target)
    def _():
        for h in range(2):
            for d in range(RING):
                q = turn(z, d)
                if h == 0 and d == 0:
                    pltpu.make_async_copy(x3, spot(0, z), local.at[0]).wait()
                else:
                    pltpu.make_async_remote_copy(
                        src_ref=x3, dst_ref=spot(h, q), send_sem=send.at[0], recv_sem=recv.at[h * RING + q], device_id={"z": z}, device_id_type=MESH
                    ).wait_recv()

    for n, (src, h, i, zz) in enumerate(jobs):
        stay = (i == x) & (zz == z)
        go = pltpu.make_async_remote_copy(
            src_ref=src, dst_ref=spot(h, z), send_sem=send.at[n], recv_sem=recv.at[h * RING + z], device_id={"z": zz, "x": i}, device_id_type=MESH
        )
        pl.when(jnp.logical_not(stay))(lambda go=go: go.wait_send())


def by_zy(mat):
    n = mat.shape[1]
    return mat.reshape(RING, RING, SUB, n).transpose(1, 0, 2, 3).reshape(RING * RING, SUB, n)


def invert(t):
    x, k = lax.axis_index("x"), lax.axis_index("core")
    inner = (x == 1) | (x == 2)
    dma2 = pltpu.SemaphoreType.DMA((2,))
    leaf, tile = (LEAF, LEAF), (2 * LEAF, LEAF)
    dma4 = pltpu.SemaphoreType.DMA((4,))
    dg, dq, c3, c4 = call(
        diagonal, [tile, (2 * LEAF, SUB), (LEAF, SUB), (LEAF, 2 * SUB)], [pltpu.VMEM(leaf, F32)] * 13 + sems(40) + [dma4], 1, t
    )
    team_d, hop, rows3, g3 = call(
        spread, [(8, 2 * LEAF, SUB), (LEAF, SUB), (RING, RING, LEAF, SUB), (RING, RING, LEAF, SUB)], sems(42) + [dma4], 2, dq, c3
    )
    g3 = g3.reshape(16, LEAF, SUB)
    c4, team_d = lax.optimization_barrier((c4, team_d))
    g4 = lax.all_gather(c4, ("z", "y"), axis=0)
    rows3 = rows3.reshape(16, LEAF, SUB)

    ds = lax.dynamic_slice_in_dim(team_d, jnp.where(inner, 0, 4), 2, axis=0).reshape(4 * LEAF, SUB)
    t3 = dot_blocks(g3, by_zy(ds))
    (t3_full,) = call(swap, [(4, LEAF, SUB)], sems(3) + [dma2], 3, t3)
    x3 = -dot_blocks(rows3, by_zy(t3_full.reshape(4 * LEAF, SUB)))

    (team_x,) = call(team_only, [(8, LEAF, SUB)], sems(9) + [dma2], 4, x3)
    d0 = team_d[0:2].reshape(4 * LEAF, SUB)
    d1 = team_d[2:4].reshape(4 * LEAF, SUB)
    x10s = jnp.concatenate([team_x[2], team_x[4], team_x[3], team_x[5]], axis=0)
    a_top = jnp.concatenate([d0, jnp.zeros_like(d0)], axis=1)
    a_bot = jnp.concatenate([x10s, d1], axis=1)
    a_mat = jnp.concatenate([a_top, a_bot], axis=0).reshape(2, RING, 2, 2 * SUB, 2 * SUB)
    a_blocks = jnp.stack([a_mat[0, :, 0], a_mat[1, :, 0], a_mat[1, :, 1], a_mat[0, :, 1]]).reshape(16, 2 * SUB, 2 * SUB)
    t4 = dot_blocks(g4, a_blocks)
    d2_rows = jnp.where(x == 2, lax.dynamic_index_in_dim(team_d, 4 + k, axis=0, keepdims=False)[:LEAF], hop)
    first_rows = jnp.where(inner, d2_rows, x3)
    team_t, rows4 = call(team_and_plane, [(8, LEAF, 2 * SUB), (RING, RING, LEAF, SUB)], sems(25) + [dma2], 5, t4, first_rows)
    rows4 = rows4.reshape(16, LEAF, SUB)
    t_first = jnp.concatenate([team_t[4], team_t[2], team_t[5], team_t[3]], axis=0)
    t_second = jnp.where(inner, 0.0, jnp.concatenate([team_t[6], team_t[0], team_t[7], team_t[1]], axis=0))
    x4 = -(dot_blocks(rows4, by_zy(t_first)) + dot_blocks(rows3, by_zy(t_second)))
    (out,) = call(place, [tile], [pltpu.SemaphoreType.DMA((3,)), pltpu.SemaphoreType.DMA((8,)), dma2], 6, dg, x3, x4)
    return out


def solution(mesh):
    grid = Mesh(mesh.devices.reshape(RING, RING, RING, 2), AXES)
    spec = P(("x", "core"), ("z", "y"))
    return jax.shard_map(invert, mesh=grid, in_specs=(spec,), out_specs=spec, check_vma=False)
```
